32 devices in a mesh: grp: 16 (over z, x, core), mode: 2 (over y).
Axes of the slice: x: 2, y: 2, z: 4, core: 2. Of those that a mesh axis runs over, the one named last changes fastest.
Arguments:
- probe: float32 [2, 8, 512, 512], P(None, 'mode'), may hold values from -3 to 3
- prev_direction: float32 [2, 8, 512, 512], P(None, 'mode'), may hold values from -0.6 to 0.6
- prev_norm: float32 [8], P('mode'), may hold values from 0.5 to 4
- object_tile: bfloat16 [2, 10240, 640], P(None, 'grp'), may hold values from -4 to 4
- offsets: int32 [32, 2], P('grp'), may hold values from 0 to 128
- amplitude: bfloat16 [32, 512, 512], P('grp'), may hold values from 0.5 to 3.5
Outputs:
- new_probe: float32 [2, 8, 512, 512], P(None, 'mode')
- new_direction: float32 [2, 8, 512, 512], P(None, 'mode')
- new_norm: float32 [8], P('mode')
The draws below stay inside these ranges and needn't reach their ends.
All inputs are finite; a program needn't handle non-finite values.
Results may differ from the reference program's by a relative error of at most 0.0045.
Values sent between devices are 32-bit elements; how exact they have to be, the bound alone decides.
A program may use at most 128 MiB of HBM per device.

```python
import math
import jax
import jax.numpy as jnp
from jax import lax

M = 8
N = 512
POS_DEV = 2
SPAN = 128
OBJ = 640
POSITIONS = 32
N_GRP = 16


def draw_object_tile(key, part):
    phase_key = jax.random.fold_in(key, 11)
    value_key = jax.random.fold_in(key, 12)
    phases = jax.random.uniform(phase_key, (N_GRP,), jnp.float32, 0.0, 2.0 * math.pi)
    rows = jnp.arange(N_GRP * OBJ, dtype=jnp.int32)
    local = (rows % OBJ).astype(jnp.float32)
    group = rows // OBJ
    shift = jnp.sum(jnp.where(group[:, None] == jnp.arange(N_GRP, dtype=jnp.int32)[None, :], phases[None, :], 0.0), axis=1)
    envelope = jnp.exp(0.9 * jnp.sin(2.0 * math.pi * local / OBJ + shift))
    values = 0.7 * jax.random.normal(value_key, (2, N_GRP * OBJ, OBJ), jnp.float32)
    values = jnp.clip(values * envelope[None, :, None], -4.0, 4.0)
    return values.astype(jnp.bfloat16)


def plant(values, rng, smallest, top_value):
    index_at = [jax.random.randint(jax.random.fold_in(rng, axis), (), 0, length) for axis, length in enumerate(values.shape)]
    longest = values.shape.index(max(values.shape))
    beside = index_at[:longest] + [(index_at[longest] + 1) % values.shape[longest]] + index_at[longest + 1:]
    return values.at[tuple(index_at)].set(smallest).at[tuple(beside)].set(top_value)


def shard_levels(stream_key, dims, cuts, smallest, largest):
    def one(dim, parts):
        steps = jax.random.uniform(jax.random.fold_in(jax.random.fold_in(stream_key, 6), dim), (parts,), jnp.float32, smallest / len(cuts), largest / len(cuts))
        return jnp.repeat(jnp.exp(steps), dims[dim] // parts).reshape((-1,) + (1,) * (len(dims) - dim - 1))

    gain = one(*cuts[0])
    for cut in cuts[1:]:
        gain = gain * one(*cut)
    return gain


def gaussian(stream_key, shape, spread, reach, shards=(), held_as=jnp.bfloat16):
    drawn = jax.random.normal(stream_key, shape, jnp.float32) * spread
    if len(shards) > 0:
        drawn = shard_levels(stream_key, shape, shards, -0.22, 0.18) * drawn
    return jnp.clip(drawn, min=-reach, max=reach).astype(held_as)


def setup_inputs(seed: int = 0) -> dict:
    keys = jax.random.split(jax.random.key(seed), 7)
    probe = gaussian(keys[0], (2, M, N, N), 0.5, 3.0, ((1, 2),), jnp.float32)
    prev_direction = gaussian(keys[1], (2, M, N, N), 0.1, 0.6, ((1, 2),), jnp.float32)
    prev_norm = jnp.clip(jnp.exp(math.log(4.0) - 2.0794415 * jax.random.uniform(keys[2], (M,), jnp.float32) ** shard_levels(keys[2], (M,), ((0, 2),), -0.2, 0.2)), 0.5, 4.0)
    object_tile = draw_object_tile(jax.random.fold_in(keys[6], 71), 0)
    offsets = plant(jax.random.randint(keys[4], (POSITIONS, 2), 0, SPAN + 1), jax.random.fold_in(keys[4], 1), 0, SPAN).astype(jnp.int32)
    amplitude = jnp.clip(0.5 + 3.0 * jax.random.uniform(keys[5], (POSITIONS, N, N), jnp.float32) ** shard_levels(keys[5], (POSITIONS, N, N), ((0, 16),), -0.2, 0.2), 0.5, 3.5).astype(jnp.bfloat16)
    return {"probe": probe, "prev_direction": prev_direction, "prev_norm": prev_norm, "object_tile": object_tile, "offsets": offsets, "amplitude": amplitude}


def tables(width, sign):
    index = jnp.arange(width, dtype=jnp.int32)
    product = index[:, None] * index[None, :] % width
    angle = -2.0 * math.pi / width * product.astype(jnp.float32)
    scale = 1.0 / math.sqrt(width)
    real_part = (jnp.cos(angle) * scale).astype(jnp.bfloat16)
    imag_part = (sign * jnp.sin(angle) * scale).astype(jnp.bfloat16)
    right = jnp.concatenate([jnp.concatenate([real_part, imag_part], 1), jnp.concatenate([-imag_part, real_part], 1)], 0)
    left = jnp.concatenate([jnp.concatenate([real_part, -imag_part], 1), jnp.concatenate([imag_part, real_part], 1)], 0)
    return (right, left)

def transform(real_in, imag_in, right, left):
    count, width = (real_in.shape[0], real_in.shape[1])
    joined = jnp.concatenate([real_in, imag_in], axis=2).reshape(count * width, 2 * width)
    half = jnp.dot(joined.astype(jnp.float32), right.astype(jnp.float32), preferred_element_type=jnp.float32)
    half = half.astype(jnp.bfloat16).reshape(count, width, 2 * width)
    stacked = jnp.concatenate([half[:, :, :width], half[:, :, width:]], axis=1)
    out = jnp.einsum('ab,mbc->mac', left.astype(jnp.float32), stacked.astype(jnp.float32))
    return (out[:, :width], out[:, width:])

def reference(probe, prev_direction, prev_norm, object_tile, offsets, amplitude):
    fwd_right, fwd_left = tables(N, 1.0)
    inv_right, inv_left = tables(N, -1.0)
    probe_re, probe_im = (probe[0], probe[1])

    def visit(carry, index):
        grad_re, grad_im, illum = carry
        group = index // POS_DEV
        row = (group * OBJ + offsets[index, 0]).astype(jnp.int32)
        col = offsets[index, 1].astype(jnp.int32)
        patch = lax.dynamic_slice(object_tile, (jnp.int32(0), row, col), (2, N, N)).astype(jnp.float32)
        obj_re, obj_im = (patch[0], patch[1])
        exit_re = (probe_re * obj_re - probe_im * obj_im).astype(jnp.bfloat16)
        exit_im = (probe_re * obj_im + probe_im * obj_re).astype(jnp.bfloat16)
        wave_re, wave_im = transform(exit_re, exit_im, fwd_right, fwd_left)
        intensity = lax.optimization_barrier(jnp.sum(wave_re * wave_re + wave_im * wave_im, axis=0))
        ratio = amplitude[index].astype(jnp.float32) / jnp.sqrt(intensity + 1.0)
        fixed_re = (ratio * wave_re).astype(jnp.bfloat16)
        fixed_im = (ratio * wave_im).astype(jnp.bfloat16)
        back_re, back_im = transform(fixed_re, fixed_im, inv_right, inv_left)
        diff_re = back_re - exit_re.astype(jnp.float32)
        diff_im = back_im - exit_im.astype(jnp.float32)
        grad_re = grad_re + obj_re * diff_re + obj_im * diff_im
        grad_im = grad_im + obj_re * diff_im - obj_im * diff_re
        illum = illum + obj_re * obj_re + obj_im * obj_im
        return ((grad_re, grad_im, illum), None)
    start = (jnp.zeros((M, N, N), jnp.float32), jnp.zeros((M, N, N), jnp.float32), jnp.zeros((N, N), jnp.float32))
    (grad_re, grad_im, illum), unused = lax.scan(visit, start, jnp.arange(POSITIONS, dtype=jnp.int32))
    total = jnp.sum(illum)
    denom = illum + total / (N * N)
    pre_re = grad_re / denom
    pre_im = grad_im / denom
    new_norm = lax.optimization_barrier(jnp.mean(grad_re * pre_re + grad_im * pre_im, axis=(1, 2)))
    beta = (new_norm / prev_norm)[:, None, None]
    dir_re = pre_re + beta * prev_direction[0]
    dir_im = pre_im + beta * prev_direction[1]
    upper = lax.optimization_barrier(jnp.mean(grad_re * dir_re + grad_im * dir_im, axis=(1, 2)))
    lower = lax.optimization_barrier(jnp.mean(illum * (dir_re * dir_re + dir_im * dir_im), axis=(1, 2)))
    alpha = (upper / (lower + 1.0))[:, None, None]
    new_direction = jnp.stack([dir_re, dir_im])
    new_probe = jnp.stack([probe_re + alpha * dir_re, probe_im + alpha * dir_im])
    return (new_probe, new_direction, new_norm)
```

```python
import functools
import math

import jax
import jax.numpy as jnp
from jax import lax
from jax.experimental import pallas as pl
from jax.experimental.pallas import tpu as pltpu
from jax.sharding import PartitionSpec as P

VMEM_LIMIT = 60 * 1024 * 1024
TILE = 256


def base_table(width):
    index = jnp.arange(width, dtype=jnp.int32)
    product = index[:, None] * index[None, :] % width
    angle = -2.0 * math.pi / width * product.astype(jnp.float32)
    scale = 1.0 / math.sqrt(width)
    real_part = (jnp.cos(angle) * scale).astype(jnp.bfloat16)
    imag_part = (jnp.sin(angle) * scale).astype(jnp.bfloat16)
    return jnp.stack([real_part, imag_part])


def build_pair(base_ref, plus, minus):
    width = base_ref.shape[1]
    cosine, sine = base_ref[0], base_ref[1]
    for ref, sign in ((plus, 1), (minus, -1)):
        ref[:width, :width] = cosine
        ref[width:, width:] = cosine
        ref[:width, width:] = sine if sign > 0 else -sine
        ref[width:, :width] = -sine if sign > 0 else sine


def transform(joined, stacked, right, left, emit):
    width = joined.shape[0]
    tile = min(TILE, width)

    def first(step, carry):
        at = pl.multiple_of(step * tile, tile)
        half = jnp.dot(joined[pl.ds(at, tile), :], right[...], preferred_element_type=jnp.float32)
        half = half.astype(jnp.bfloat16)
        stacked[pl.ds(at, tile), :] = half[:, :width]
        stacked[pl.ds(at + width, tile), :] = half[:, width:]
        return carry

    def second(step, carry):
        at = pl.multiple_of(step * tile, tile)
        rows = pl.ds(at, tile)
        real = jnp.dot(left[rows, :], stacked[...], preferred_element_type=jnp.float32)
        imag = jnp.dot(left[pl.ds(at + width, tile), :], stacked[...], preferred_element_type=jnp.float32)
        emit(rows, real, imag)
        return carry

    lax.fori_loop(0, width // tile, first, 0)
    lax.fori_loop(0, width // tile, second, 0)


def forward_kernel(base_ref, probe_ref, patch_ref, wave_ref, exit_ref, sum_ref, plus, minus, joined, stacked):
    mode = pl.program_id(0)
    width = sum_ref.shape[0]
    tile = 64

    @pl.when(mode == 0)
    def _():
        build_pair(base_ref, plus, minus)
        sum_ref[...] = jnp.zeros_like(sum_ref)

    def leave(step, carry):
        rows = pl.ds(pl.multiple_of(step * tile, tile), tile)
        obj_re = patch_ref[0, rows, :].astype(jnp.float32)
        obj_im = patch_ref[1, rows, :].astype(jnp.float32)
        pro_re, pro_im = probe_ref[0, 0, rows, :], probe_ref[1, 0, rows, :]
        exit_re = (pro_re * obj_re - pro_im * obj_im).astype(jnp.bfloat16)
        exit_im = (pro_re * obj_im + pro_im * obj_re).astype(jnp.bfloat16)
        joined[rows, :width] = exit_re
        joined[rows, width:] = exit_im
        exit_ref[0, 0, rows, :] = exit_re
        exit_ref[0, 1, rows, :] = exit_im
        return carry

    lax.fori_loop(0, width // tile, leave, 0)

    def emit(rows, real, imag):
        wave_ref[0, 0, rows, :] = real
        wave_ref[0, 1, rows, :] = imag
        sum_ref[rows, :] += real * real + imag * imag

    transform(joined, stacked, plus, minus, emit)


def backward_kernel(first, base_ref, total_ref, amp_ref, wave_ref, exit_ref, patch_ref, *rest):
    if first:
        grad_in, (grad_ref, plus, minus, joined, stacked, ratio) = None, rest
    else:
        grad_in, grad_ref, plus, minus, joined, stacked, ratio = rest
    width = total_ref.shape[0]
    tile = 64

    @pl.when(pl.program_id(0) == 0)
    def _():
        build_pair(base_ref, plus, minus)

        def scale(step, carry):
            rows = pl.ds(pl.multiple_of(step * tile, tile), tile)
            ratio[rows, :] = amp_ref[0, rows, :].astype(jnp.float32) / jnp.sqrt(total_ref[rows, :] + 1.0)
            return carry

        lax.fori_loop(0, width // tile, scale, 0)

    def fix(step, carry):
        rows = pl.ds(pl.multiple_of(step * tile, tile), tile)
        joined[rows, :width] = (ratio[rows, :] * wave_ref[0, 0, rows, :]).astype(jnp.bfloat16)
        joined[rows, width:] = (ratio[rows, :] * wave_ref[0, 1, rows, :]).astype(jnp.bfloat16)
        return carry

    lax.fori_loop(0, width // tile, fix, 0)

    def emit(rows, real, imag):
        obj_re = patch_ref[0, rows, :].astype(jnp.float32)
        obj_im = patch_ref[1, rows, :].astype(jnp.float32)
        diff_re = real - exit_ref[0, 0, rows, :].astype(jnp.float32)
        diff_im = imag - exit_ref[0, 1, rows, :].astype(jnp.float32)
        add_re = obj_re * diff_re + obj_im * diff_im
        add_im = obj_re * diff_im - obj_im * diff_re
        if grad_in is not None:
            add_re = grad_in[0, 0, rows, :] + add_re
            add_im = grad_in[0, 1, rows, :] + add_im
        grad_ref[0, 0, rows, :] = add_re
        grad_ref[0, 1, rows, :] = add_im

    transform(joined, stacked, minus, plus, emit)


def finish_kernel(mode, norm_ref, grad_ref, illum_ref, probe_ref, dir_ref, *rest):
    new_probe, new_dir, new_norm = rest[-4:-1]
    denom = rest[-1]
    width = illum_ref.shape[0]
    tile = 32
    steps = width // tile
    pixels = float(width * width)

    def rows_of(step):
        return pl.ds(pl.multiple_of(step * tile, tile), tile)

    def fold(block):
        return jnp.sum(block.reshape(tile // 8, 8, width), axis=0)

    zero = jnp.zeros((8, width), jnp.float32)
    total = jnp.sum(lax.fori_loop(0, steps, lambda i, acc: acc + fold(illum_ref[rows_of(i), :]), zero))
    shift = total / pixels

    def one(step, acc):
        rows = rows_of(step)
        den = illum_ref[rows, :] + shift
        g_re, g_im = grad_ref[0, 0, rows, :], grad_ref[0, 1, rows, :]
        p_re, p_im = g_re / den, g_im / den
        new_dir[0, 0, rows, :] = p_re
        new_dir[1, 0, rows, :] = p_im
        return acc + fold(g_re * p_re + g_im * p_im)

    norm = jnp.sum(lax.fori_loop(0, steps, one, zero)) / pixels
    new_norm[0, 0] = norm
    beta = norm / norm_ref[mode]

    def two(step, acc):
        rows = rows_of(step)
        upper, lower = acc
        d_re = new_dir[0, 0, rows, :] + beta * dir_ref[0, 0, rows, :]
        d_im = new_dir[1, 0, rows, :] + beta * dir_ref[1, 0, rows, :]
        new_dir[0, 0, rows, :] = d_re
        new_dir[1, 0, rows, :] = d_im
        upper = upper + fold(grad_ref[0, 0, rows, :] * d_re + grad_ref[0, 1, rows, :] * d_im)
        lower = lower + fold(illum_ref[rows, :] * (d_re * d_re + d_im * d_im))
        return (upper, lower)

    upper, lower = lax.fori_loop(0, steps, two, (zero, zero))
    alpha = (jnp.sum(upper) / pixels) / (jnp.sum(lower) / pixels + 1.0)

    def three(step, carry):
        rows = rows_of(step)
        new_probe[0, 0, rows, :] = probe_ref[0, 0, rows, :] + alpha * new_dir[0, 0, rows, :]
        new_probe[1, 0, rows, :] = probe_ref[1, 0, rows, :] + alpha * new_dir[1, 0, rows, :]
        return carry

    lax.fori_loop(0, steps, three, 0)


def whole(shape):
    return pl.BlockSpec(shape, lambda *_: (0,) * len(shape))


def table_scratch(width):
    return [
        pltpu.VMEM((2 * width, 2 * width), jnp.bfloat16),
        pltpu.VMEM((2 * width, 2 * width), jnp.bfloat16),
        pltpu.VMEM((width, 2 * width), jnp.bfloat16),
        pltpu.VMEM((2 * width, width), jnp.bfloat16),
    ]


def params():
    return pltpu.CompilerParams(dimension_semantics=("arbitrary",), vmem_limit_bytes=VMEM_LIMIT)


def cost(modes, width, moved):
    return pl.CostEstimate(flops=modes * 16 * width**3, bytes_accessed=moved, transcendentals=0)


def forward(base, probe, patch):
    modes, width = probe.shape[1], probe.shape[2]
    return pl.pallas_call(
        forward_kernel,
        grid=(modes,),
        in_specs=[
            whole(base.shape),
            pl.BlockSpec((2, 1, width, width), lambda m: (0, m, 0, 0)),
            whole(patch.shape),
        ],
        out_specs=[
            pl.BlockSpec((1, 2, width, width), lambda m: (m, 0, 0, 0)),
            pl.BlockSpec((1, 2, width, width), lambda m: (m, 0, 0, 0)),
            whole((width, width)),
        ],
        out_shape=[
            jax.ShapeDtypeStruct((modes, 2, width, width), jnp.float32),
            jax.ShapeDtypeStruct((modes, 2, width, width), jnp.bfloat16),
            jax.ShapeDtypeStruct((width, width), jnp.float32),
        ],
        scratch_shapes=table_scratch(width),
        compiler_params=params(),
        cost_estimate=cost(modes, width, modes * width * width * 20),
        name="forward",
    )(base, probe, patch)


def backward(base, total, amplitude, index, wave, exits, patch, grad, start, count):
    width = total.shape[0]
    at = lambda m: (m + start, 0, 0, 0)
    block = (1, 2, width, width)
    operands = [base, total, amplitude, wave, exits, patch]
    in_specs = [
        whole(base.shape),
        whole(total.shape),
        pl.BlockSpec((1, width, width), lambda m: (index, 0, 0)),
        pl.BlockSpec(block, at),
        pl.BlockSpec(block, at),
        whole(patch.shape),
    ]
    if grad is not None:
        operands.append(grad)
        in_specs.append(pl.BlockSpec(block, at))
    return pl.pallas_call(
        functools.partial(backward_kernel, grad is None),
        grid=(count,),
        in_specs=in_specs,
        out_specs=pl.BlockSpec(block, lambda m: (m, 0, 0, 0)),
        out_shape=jax.ShapeDtypeStruct((count, 2, width, width), jnp.float32),
        scratch_shapes=table_scratch(width) + [pltpu.VMEM((width, width), jnp.float32)],
        compiler_params=params(),
        cost_estimate=cost(count, width, count * width * width * 24),
        name="backward",
    )(*operands)


def finish(mode, prev_norm, grad, illum, probe, direction, outs):
    width = illum.shape[0]
    block = pl.BlockSpec((2, 1, width, width), lambda m: (0, mode, 0, 0))
    operands = [prev_norm, grad, illum, probe, direction]
    in_specs = [
        pl.BlockSpec(memory_space=pltpu.SMEM),
        whole(grad.shape),
        whole(illum.shape),
        block,
        block,
    ]
    aliases = {}
    if outs is not None:
        aliases = {len(operands): 0, len(operands) + 1: 1}
        operands += list(outs)
        in_specs += [pl.BlockSpec(memory_space=pl.ANY)] * 2
    return pl.pallas_call(
        functools.partial(finish_kernel, mode),
        grid=(1,),
        in_specs=in_specs,
        out_specs=[block, block, pl.BlockSpec(memory_space=pltpu.SMEM)],
        out_shape=[
            jax.ShapeDtypeStruct(probe.shape, jnp.float32),
            jax.ShapeDtypeStruct(probe.shape, jnp.float32),
            jax.ShapeDtypeStruct((1, 1), jnp.float32),
        ],
        scratch_shapes=[pltpu.VMEM((8, 128), jnp.float32)],
        input_output_aliases=aliases,
        compiler_params=params(),
        cost_estimate=pl.CostEstimate(flops=width * width * 30, bytes_accessed=width * width * 44, transcendentals=0),
        name="finish",
    )(*operands)


def on_device(probe, prev_direction, prev_norm, object_tile, offsets, amplitude):
    width = probe.shape[2]
    modes = probe.shape[1]
    positions = amplitude.shape[0]
    base = base_table(width)
    illum = jnp.zeros((width, width), jnp.float32)
    patches, kept = [], []
    for index in range(positions):
        patch = lax.dynamic_slice(
            object_tile, (jnp.int32(0), offsets[index, 0], offsets[index, 1]), (2, width, width)
        )
        patches.append(patch)
        wave, exits, local_sum = forward(base, probe, patch)
        if kept:
            local_sum, earlier = lax.optimization_barrier((local_sum, kept[-1][2]))
            kept[-1] = (kept[-1][0], kept[-1][1], earlier)
        total = lax.psum(local_sum, "mode")
        kept.append((wave, exits, total))
        wide = patch.astype(jnp.float32)
        illum = illum + wide[0] * wide[0] + wide[1] * wide[1]
    grad = None
    for index in range(positions - 1):
        wave, exits, total = kept[index]
        grad = backward(base, total, amplitude, index, wave, exits, patches[index], grad, 0, modes)
    wave, exits, total = kept[-1]
    sums = []
    for mode in range(modes):
        part = backward(base, total, amplitude, positions - 1, wave, exits, patches[-1], grad, mode, 1)
        if mode == 0:
            part, illum = lax.psum((part, illum), "grp")
        else:
            part, sums[-1] = lax.optimization_barrier((part, sums[-1]))
            part = lax.psum(part, "grp")
        sums.append(part)
    outs, norms = None, []
    for mode in range(modes):
        *outs, norm = finish(mode, prev_norm, sums[mode], illum, probe, prev_direction, outs)
        norms.append(norm.reshape(1))
    return (outs[0], outs[1], jnp.concatenate(norms))


def solution(mesh):
    return jax.shard_map(
        on_device,
        mesh=mesh,
        in_specs=(
            P(None, "mode", None, None),
            P(None, "mode", None, None),
            P("mode"),
            P(None, "grp", None),
            P("grp", None),
            P("grp", None, None),
        ),
        out_specs=(P(None, "mode", None, None), P(None, "mode", None, None), P("mode")),
        check_vma=False,
    )
```

```python
import functools
import math

import jax
import jax.numpy as jnp
from jax import lax
from jax.experimental import pallas as pl
from jax.experimental.pallas import tpu as pltpu
from jax.sharding import PartitionSpec as P

VMEM_LIMIT = 60 * 1024 * 1024
TILE = 256


def base_table(width):
    index = jnp.arange(width, dtype=jnp.int32)
    product = index[:, None] * index[None, :] % width
    angle = -2.0 * math.pi / width * product.astype(jnp.float32)
    scale = 1.0 / math.sqrt(width)
    real_part = (jnp.cos(angle) * scale).astype(jnp.bfloat16)
    imag_part = (jnp.sin(angle) * scale).astype(jnp.bfloat16)
    return jnp.stack([real_part, imag_part])


def build_pair(base_ref, plus, minus):
    width = base_ref.shape[1]
    cosine, sine = base_ref[0], base_ref[1]
    for ref, sign in ((plus, 1), (minus, -1)):
        ref[:width, :width] = cosine
        ref[width:, width:] = cosine
        ref[:width, width:] = sine if sign > 0 else -sine
        ref[width:, :width] = -sine if sign > 0 else sine


def transform(joined, stacked, right, left, emit):
    width = joined.shape[0]
    tile = min(TILE, width)

    def first(step, carry):
        at = pl.multiple_of(step * tile, tile)
        half = jnp.dot(joined[pl.ds(at, tile), :], right[...], preferred_element_type=jnp.float32)
        half = half.astype(jnp.bfloat16)
        stacked[pl.ds(at, tile), :] = half[:, :width]
        stacked[pl.ds(at + width, tile), :] = half[:, width:]
        return carry

    def second(step, carry):
        at = pl.multiple_of(step * tile, tile)
        rows = pl.ds(at, tile)
        real = jnp.dot(left[rows, :], stacked[...], preferred_element_type=jnp.float32)
        imag = jnp.dot(left[pl.ds(at + width, tile), :], stacked[...], preferred_element_type=jnp.float32)
        emit(rows, real, imag)
        return carry

    lax.fori_loop(0, width // tile, first, 0)
    lax.fori_loop(0, width // tile, second, 0)


def forward_kernel(base_ref, probe_ref, patch_ref, wave_ref, exit_ref, sum_ref, plus, minus, joined, stacked):
    mode = pl.program_id(0)
    width = sum_ref.shape[0]
    tile = 64

    @pl.when(mode == 0)
    def _():
        build_pair(base_ref, plus, minus)
        sum_ref[...] = jnp.zeros_like(sum_ref)

    def leave(step, carry):
        rows = pl.ds(pl.multiple_of(step * tile, tile), tile)
        obj_re = patch_ref[0, rows, :].astype(jnp.float32)
        obj_im = patch_ref[1, rows, :].astype(jnp.float32)
        pro_re, pro_im = probe_ref[0, 0, rows, :], probe_ref[1, 0, rows, :]
        exit_re = (pro_re * obj_re - pro_im * obj_im).astype(jnp.bfloat16)
        exit_im = (pro_re * obj_im + pro_im * obj_re).astype(jnp.bfloat16)
        joined[rows, :width] = exit_re
        joined[rows, width:] = exit_im
        exit_ref[0, 0, rows, :] = exit_re
        exit_ref[0, 1, rows, :] = exit_im
        return carry

    lax.fori_loop(0, width // tile, leave, 0)

    def emit(rows, real, imag):
        wave_ref[0, 0, rows, :] = real
        wave_ref[0, 1, rows, :] = imag
        sum_ref[rows, :] += real * real + imag * imag

    transform(joined, stacked, plus, minus, emit)


def backward_kernel(first, base_ref, total_ref, amp_ref, wave_ref, exit_ref, patch_ref, *rest):
    if first:
        grad_in, (grad_ref, plus, minus, joined, stacked, ratio) = None, rest
    else:
        grad_in, grad_ref, plus, minus, joined, stacked, ratio = rest
    width = total_ref.shape[0]
    tile = 64

    @pl.when(pl.program_id(0) == 0)
    def _():
        build_pair(base_ref, plus, minus)

        def scale(step, carry):
            rows = pl.ds(pl.multiple_of(step * tile, tile), tile)
            ratio[rows, :] = amp_ref[0, rows, :].astype(jnp.float32) / jnp.sqrt(total_ref[rows, :] + 1.0)
            return carry

        lax.fori_loop(0, width // tile, scale, 0)

    def fix(step, carry):
        rows = pl.ds(pl.multiple_of(step * tile, tile), tile)
        joined[rows, :width] = (ratio[rows, :] * wave_ref[0, 0, rows, :]).astype(jnp.bfloat16)
        joined[rows, width:] = (ratio[rows, :] * wave_ref[0, 1, rows, :]).astype(jnp.bfloat16)
        return carry

    lax.fori_loop(0, width // tile, fix, 0)

    def emit(rows, real, imag):
        obj_re = patch_ref[0, rows, :].astype(jnp.float32)
        obj_im = patch_ref[1, rows, :].astype(jnp.float32)
        diff_re = real - exit_ref[0, 0, rows, :].astype(jnp.float32)
        diff_im = imag - exit_ref[0, 1, rows, :].astype(jnp.float32)
        add_re = obj_re * diff_re + obj_im * diff_im
        add_im = obj_re * diff_im - obj_im * diff_re
        if grad_in is not None:
            add_re = grad_in[0, 0, rows, :] + add_re
            add_im = grad_in[0, 1, rows, :] + add_im
        grad_ref[0, 0, rows, :] = add_re
        grad_ref[0, 1, rows, :] = add_im

    transform(joined, stacked, minus, plus, emit)


def finish_kernel(norm_ref, grad_ref, illum_ref, probe_ref, dir_ref, new_probe, new_dir, new_norm):
    mode = pl.program_id(0)
    width = illum_ref.shape[0]
    tile = 32
    steps = width // tile
    pixels = float(width * width)

    def rows_of(step):
        return pl.ds(pl.multiple_of(step * tile, tile), tile)

    def fold(block):
        return jnp.sum(block.reshape(tile // 8, 8, width), axis=0)

    zero = jnp.zeros((8, width), jnp.float32)
    total = jnp.sum(lax.fori_loop(0, steps, lambda i, acc: acc + fold(illum_ref[rows_of(i), :]), zero))
    shift = total / pixels

    def one(step, acc):
        rows = rows_of(step)
        den = illum_ref[rows, :] + shift
        g_re, g_im = grad_ref[0, 0, rows, :], grad_ref[0, 1, rows, :]
        p_re, p_im = g_re / den, g_im / den
        new_dir[0, 0, rows, :] = p_re
        new_dir[1, 0, rows, :] = p_im
        return acc + fold(g_re * p_re + g_im * p_im)

    norm = jnp.sum(lax.fori_loop(0, steps, one, zero)) / pixels
    new_norm[mode] = norm
    beta = norm / norm_ref[mode]

    def two(step, acc):
        rows = rows_of(step)
        upper, lower = acc
        d_re = new_dir[0, 0, rows, :] + beta * dir_ref[0, 0, rows, :]
        d_im = new_dir[1, 0, rows, :] + beta * dir_ref[1, 0, rows, :]
        new_dir[0, 0, rows, :] = d_re
        new_dir[1, 0, rows, :] = d_im
        upper = upper + fold(grad_ref[0, 0, rows, :] * d_re + grad_ref[0, 1, rows, :] * d_im)
        lower = lower + fold(illum_ref[rows, :] * (d_re * d_re + d_im * d_im))
        return (upper, lower)

    upper, lower = lax.fori_loop(0, steps, two, (zero, zero))
    alpha = (jnp.sum(upper) / pixels) / (jnp.sum(lower) / pixels + 1.0)

    def three(step, carry):
        rows = rows_of(step)
        new_probe[0, 0, rows, :] = probe_ref[0, 0, rows, :] + alpha * new_dir[0, 0, rows, :]
        new_probe[1, 0, rows, :] = probe_ref[1, 0, rows, :] + alpha * new_dir[1, 0, rows, :]
        return carry

    lax.fori_loop(0, steps, three, 0)


def whole(shape):
    return pl.BlockSpec(shape, lambda *_: (0,) * len(shape))


def table_scratch(width):
    return [
        pltpu.VMEM((2 * width, 2 * width), jnp.bfloat16),
        pltpu.VMEM((2 * width, 2 * width), jnp.bfloat16),
        pltpu.VMEM((width, 2 * width), jnp.bfloat16),
        pltpu.VMEM((2 * width, width), jnp.bfloat16),
    ]


def params():
    return pltpu.CompilerParams(dimension_semantics=("arbitrary",), vmem_limit_bytes=VMEM_LIMIT)


def cost(modes, width, moved):
    return pl.CostEstimate(flops=modes * 16 * width**3, bytes_accessed=moved, transcendentals=0)


def forward(base, probe, patch):
    modes, width = probe.shape[1], probe.shape[2]
    return pl.pallas_call(
        forward_kernel,
        grid=(modes,),
        in_specs=[
            whole(base.shape),
            pl.BlockSpec((2, 1, width, width), lambda m: (0, m, 0, 0)),
            whole(patch.shape),
        ],
        out_specs=[
            pl.BlockSpec((1, 2, width, width), lambda m: (m, 0, 0, 0)),
            pl.BlockSpec((1, 2, width, width), lambda m: (m, 0, 0, 0)),
            whole((width, width)),
        ],
        out_shape=[
            jax.ShapeDtypeStruct((modes, 2, width, width), jnp.float32),
            jax.ShapeDtypeStruct((modes, 2, width, width), jnp.bfloat16),
            jax.ShapeDtypeStruct((width, width), jnp.float32),
        ],
        scratch_shapes=table_scratch(width),
        compiler_params=params(),
        cost_estimate=cost(modes, width, modes * width * width * 20),
        name="forward",
    )(base, probe, patch)


def backward(base, total, amplitude, index, wave, exits, patch, grad, start, count):
    width = total.shape[0]
    at = lambda m: (m + start, 0, 0, 0)
    block = (1, 2, width, width)
    operands = [base, total, amplitude, wave, exits, patch]
    in_specs = [
        whole(base.shape),
        whole(total.shape),
        pl.BlockSpec((1, width, width), lambda m: (index, 0, 0)),
        pl.BlockSpec(block, at),
        pl.BlockSpec(block, at),
        whole(patch.shape),
    ]
    if grad is not None:
        operands.append(grad)
        in_specs.append(pl.BlockSpec(block, at))
    return pl.pallas_call(
        functools.partial(backward_kernel, grad is None),
        grid=(count,),
        in_specs=in_specs,
        out_specs=pl.BlockSpec(block, lambda m: (m, 0, 0, 0)),
        out_shape=jax.ShapeDtypeStruct((count, 2, width, width), jnp.float32),
        scratch_shapes=table_scratch(width) + [pltpu.VMEM((width, width), jnp.float32)],
        compiler_params=params(),
        cost_estimate=cost(count, width, count * width * width * 24),
        name="backward",
    )(*operands)


def finish(prev_norm, grad, illum, probe, direction):
    modes, width = probe.shape[1], illum.shape[0]
    block = pl.BlockSpec((2, 1, width, width), lambda m: (0, m, 0, 0))
    return pl.pallas_call(
        finish_kernel,
        grid=(modes,),
        in_specs=[
            pl.BlockSpec(memory_space=pltpu.SMEM),
            pl.BlockSpec((1, 2, width, width), lambda m: (m, 0, 0, 0)),
            whole(illum.shape),
            block,
            block,
        ],
        out_specs=[block, block, pl.BlockSpec(memory_space=pltpu.SMEM)],
        out_shape=[
            jax.ShapeDtypeStruct(probe.shape, jnp.float32),
            jax.ShapeDtypeStruct(probe.shape, jnp.float32),
            jax.ShapeDtypeStruct((modes,), jnp.float32),
        ],
        compiler_params=params(),
        name="finish",
    )(prev_norm, grad, illum, probe, direction)


def sum_over_modes(local_sum):
    if lax.axis_size("mode") != 2:
        return lax.psum(local_sum, "mode")
    return local_sum + lax.ppermute(local_sum, "mode", [(0, 1), (1, 0)])


def on_device(probe, prev_direction, prev_norm, object_tile, offsets, amplitude):
    width = probe.shape[2]
    modes = probe.shape[1]
    positions = amplitude.shape[0]
    base = base_table(width)
    illum = jnp.zeros((width, width), jnp.float32)
    patches, kept = [], []
    for index in range(positions):
        patch = lax.dynamic_slice(
            object_tile, (jnp.int32(0), offsets[index, 0], offsets[index, 1]), (2, width, width)
        )
        patches.append(patch)
        wave, exits, local_sum = forward(base, probe, patch)
        total = sum_over_modes(local_sum)
        kept.append((wave, exits, total))
        wide = patch.astype(jnp.float32)
        illum = illum + wide[0] * wide[0] + wide[1] * wide[1]
    grad = None
    for index in range(positions - 1):
        wave, exits, total = kept[index]
        grad = backward(base, total, amplitude, index, wave, exits, patches[index], grad, 0, modes)
    wave, exits, total = kept[-1]
    part = backward(base, total, amplitude, positions - 1, wave, exits, patches[-1], grad, 0, modes)
    part, illum = lax.psum((part, illum), "grp")
    return tuple(finish(prev_norm, part, illum, probe, prev_direction))


def solution(mesh):
    return jax.shard_map(
        on_device,
        mesh=mesh,
        in_specs=(
            P(None, "mode", None, None),
            P(None, "mode", None, None),
            P("mode"),
            P(None, "grp", None),
            P("grp", None),
            P("grp", None, None),
        ),
        out_specs=(P(None, "mode", None, None), P(None, "mode", None, None), P("mode")),
        check_vma=False,
    )
```
